128 devices in a mesh: fsdp: 32 (over x_hi, z, y), tensor: 4 (over x_lo, core).
Axes of the slice: x: 4 (x_hi: 2, x_lo: 2; x = x_hi * 2 + x_lo), y: 4, z: 4, core: 2. Of those that a mesh axis runs over, the one named last changes fastest.
Arguments:
- activations: bfloat16 [32768, 5120], P('fsdp', 'tensor'), may hold values from -6 to 6
- cotangent: bfloat16 [32768, 5120], P('fsdp', 'tensor'), may hold values from -0.032958984 to 0.032958984
- weights: float32 [5120, 5120], P(None, ('tensor', 'fsdp')), may hold values from -0.025 to 0.025
- first_moment: float32 [5120, 5120], P(None, ('tensor', 'fsdp')), may hold values from -3 to 3
- second_moment: float32 [5120, 5120], P(None, ('tensor', 'fsdp')), may hold values from 0.01 to 1
Outputs:
- weights_new: float32 [5120, 5120], P('fsdp', 'tensor')
- first_new: float32 [5120, 5120], P('fsdp', 'tensor')
- second_new: float32 [5120, 5120], P('fsdp', 'tensor')
- weights_bf16: bfloat16 [5120, 5120], P(None, 'tensor')
The draws below stay inside these ranges and needn't reach their ends.
All inputs are finite; a program needn't handle non-finite values.
Results may differ from the reference program's by a relative error of at most 0.014.
Values may be sent and summed in bfloat16 or wider, within the bound.
No kernel may reach another device: no remote copies, remote signals or barrier semaphores. Data moves between devices by JAX's collectives and lax.ppermute only.
A program may use at most 128 MiB of HBM per device.

```python
import math
import jax
import jax.numpy as jnp
from jax import lax

D = 5120
TOK_DEV = 1024
STEP = 20
TOKENS = 32768
N_FSDP = 32


def with_spikes(array, key, source, target, parts, factor):
    owner, partner = [(jnp.arange(array.shape[dim]) // (array.shape[dim] // parts)).reshape([-1 if axis == dim else 1 for axis in range(array.ndim)]) for dim in (source, target)]
    chosen = jax.random.permutation(key, parts)[partner]
    strong = (owner == chosen) | (owner == (partner + parts // 2) % parts)
    return jnp.where(strong, factor * array, array)


def block_levels(key, extent, split, low, largest):
    factor_of = 1.0
    for dim, blocks in split:
        heights = jax.random.uniform(jax.random.fold_in(jax.random.fold_in(key, 6), dim), (blocks,), jnp.float32, low / len(split), largest / len(split))
        factor_of = factor_of * jnp.repeat(jnp.exp(heights), extent[dim] // blocks).reshape((-1,) + (1,) * (len(extent) - 1 - dim))
    return factor_of


def normal_values(stream_key, extent, scale, most, pieces=(), kind=jnp.bfloat16):
    array = scale * jax.random.normal(stream_key, extent, jnp.float32)
    if pieces:
        array = array * block_levels(stream_key, extent, pieces, -0.22, 0.18)
    return jnp.clip(array, -most, most).astype(kind)


def heavy_noise(own_key, dims, deviation, reach, split, heavy, dtype=jnp.bfloat16):
    values = deviation * jax.random.normal(own_key, dims, jnp.float32)
    if split:
        values = values * block_levels(own_key, dims, split, -0.22, 0.18)
    return jnp.clip(with_spikes(values, jax.random.fold_in(own_key, 3), *heavy), -reach, reach).astype(dtype)


def setup_inputs(seed: int = 0) -> dict:
    arg_keys = jax.random.split(jax.random.key(seed), 6)
    activations = heavy_noise(arg_keys[0], (TOKENS, D), 1.0, 6.0, ((0, 32), (1, 4)), (0, 1, 32, 2.75))
    cotangent = normal_values(arg_keys[1], (TOKENS, D), (1.0 / TOKENS ** 0.5), 0.032958984, ((0, 32), (1, 4)))
    weights = normal_values(arg_keys[2], (D, D), 0.004, 0.025, ((1, 128),), jnp.float32)
    first_moment = normal_values(arg_keys[3], (D, D), 0.5, 3.0, ((1, 128),), jnp.float32)
    second_moment = jnp.clip(jnp.exp(math.log(1.0) - 4.6051702 * jax.random.uniform(arg_keys[4], (D, D), jnp.float32) ** block_levels(arg_keys[4], (D, D), ((1, 128),), -0.2, 0.2)), 0.01, 1.0)
    return {"activations": activations, "cotangent": cotangent, "weights": weights, "first_moment": first_moment, "second_moment": second_moment}


beta_one = 0.9
beta_two = 0.95
adam_eps = 1e-08
learn_rate = 0.0003
decay_rate = 0.1

def adam_update(weights, first_moment, second_moment, gradient):
    first_new = beta_one * first_moment + (1.0 - beta_one) * gradient
    second_new = beta_two * second_moment + (1.0 - beta_two) * gradient * gradient
    corrected = first_new / (1.0 - beta_one ** STEP)
    scaled = jnp.sqrt(second_new / (1.0 - beta_two ** STEP)) + adam_eps
    weights_new = weights - learn_rate * (corrected / scaled + decay_rate * weights)
    return (weights_new, first_new, second_new)

def reference(activations, cotangent, weights, first_moment, second_moment):
    token_blocks = activations.reshape(N_FSDP, TOK_DEV, D)
    cotangent_blocks = cotangent.reshape(N_FSDP, TOK_DEV, D)

    def accumulate(running, block_pair):
        product = lax.dot_general(block_pair[0].astype(jnp.float32), block_pair[1].astype(jnp.float32), (((0,), (0,)), ((), ())))
        rounded = lax.optimization_barrier(product.astype(jnp.bfloat16))
        return (running + rounded.astype(jnp.float32), None)
    gradient, unused = lax.scan(accumulate, jnp.zeros((D, D), jnp.float32), (token_blocks, cotangent_blocks))
    weights_new, first_new, second_new = adam_update(weights, first_moment, second_moment, gradient)
    return (weights_new, first_new, second_new, weights_new.astype(jnp.bfloat16))
```

```python
import jax
import jax.numpy as jnp
from jax import lax
from jax.sharding import Mesh, PartitionSpec as P

STEP = 20


beta_one = 0.9
beta_two = 0.95
adam_eps = 1e-08
learn_rate = 0.0003
decay_rate = 0.1

D = 5120
ROWS = 160
COLS = 1280
FSDP = ("xh", "z", "y")


def f32(value):
    return value.astype(jnp.float32)


def bf16(value):
    return value.astype(jnp.bfloat16)


def shift(value, axis, step):
    count = lax.axis_size(axis)
    return lax.ppermute(value, axis, [(i, (i + step) % count) for i in range(count)])


def window(value, dim, start, size):
    return lax.dynamic_slice_in_dim(value, start, size, dim)


def reduce_ring(partial, axis, dim, half_dim):
    here = lax.axis_index(axis)
    half = partial.shape[half_dim] // 2

    def part(ahead, which):
        piece = window(partial, dim, (here + ahead) % 4, 1)
        return lax.slice_in_dim(piece, which * half, (which + 1) * half, axis=half_dim)

    far_up = shift(part(2, 0), axis, 1)
    far_down = shift(part(2, 1), axis, -1)
    near_up = shift(part(1, 1), axis, 1)
    near_down = shift(part(3, 0), axis, -1)
    last_up = shift(bf16(f32(part(1, 0)) + f32(far_up)), axis, 1)
    last_down = shift(bf16(f32(part(3, 1)) + f32(far_down)), axis, -1)
    low = f32(part(0, 0)) + f32(near_down) + f32(last_up)
    high = f32(part(0, 1)) + f32(near_up) + f32(last_down)
    return low, high


def reduce_plane(partial, axes):
    first = 1 if axes[0] == "y" else 0
    halves = reduce_ring(partial, axes[0], first, 1 - first)
    rows = jnp.concatenate([bf16(h) for h in halves], axis=1 - first)
    rows = rows.reshape(4, ROWS, partial.shape[-1])
    return jnp.concatenate(reduce_ring(rows, axes[1], 0, 1), axis=1)[0]


def gather_ring(block, axis, half_dim):
    half = block.shape[half_dim] // 2
    low = lax.slice_in_dim(block, 0, half, axis=half_dim)
    high = lax.slice_in_dim(block, half, 2 * half, axis=half_dim)
    low_up = shift(low, axis, 1)
    high_down = shift(high, axis, -1)
    high_up = shift(high, axis, 1)
    low_down = shift(low, axis, -1)
    far_up = shift(low_up, axis, 1)
    far_down = shift(high_down, axis, -1)
    return [
        (0, 0, block),
        (3, 0, low_up),
        (1, half, high_down),
        (3, half, high_up),
        (1, 0, low_down),
        (2, 0, far_up),
        (2, half, far_down),
    ]


def gather_plane(out, block, axes, x_half, column):
    here = lax.axis_index(axes[0])
    there = lax.axis_index(axes[1])
    line = jnp.zeros((4, *block.shape), block.dtype)
    for ahead, start, piece in gather_ring(block, axes[0], 0):
        line = lax.dynamic_update_slice(line, piece[None], ((here + ahead) % 4, start, 0))
    for ahead, start, piece in gather_ring(line, axes[1], 0):
        other = (there + ahead) % 4
        if axes[1] == "y":
            out = lax.dynamic_update_slice(out, piece[None, :, None], (x_half, start, other, 0, column))
        else:
            out = lax.dynamic_update_slice(out, piece[None, None], (x_half, other, start, 0, column))
    return out


def adam_update(weights, first_moment, second_moment, gradient):
    first_new = beta_one * first_moment + (1.0 - beta_one) * gradient
    second_new = beta_two * second_moment + (1.0 - beta_two) * gradient * gradient
    corrected = first_new / (1.0 - beta_one**STEP)
    scaled = jnp.sqrt(second_new / (1.0 - beta_two**STEP)) + adam_eps
    weights_new = weights - learn_rate * (corrected / scaled + decay_rate * weights)
    return (weights_new, first_new, second_new)


def body(activations, cotangent, weights, first_moment, second_moment):
    xh, xl, core = lax.axis_index("xh"), lax.axis_index("xl"), lax.axis_index("c")
    half = COLS // 2
    sides = ((0, ("y", "z")), (half, ("z", "y")))

    beside = shift(activations, "c", 1)
    across = shift(activations, "xl", 1)

    stacked = bf16(jnp.stack([s.T for s in (weights, first_moment, second_moment)]))
    sent = jnp.transpose(stacked.reshape(3, 40, 2, 16, ROWS), (3, 2, 0, 1, 4))
    got = lax.all_to_all(sent, ("z", "y"), 0, 0, tiled=True)

    def products(mine, other):
        lower = jnp.where(core == 0, mine, other)
        upper = jnp.where(core == 0, other, mine)
        both = jnp.concatenate([lower, upper], axis=1)
        return [
            lax.dot_general(
                both, cotangent[:, start : start + half], (((0,), (0,)), ((), ())), preferred_element_type=jnp.float32
            )
            .astype(jnp.bfloat16)
            .reshape(4, 4, ROWS, half)
            for start, _ in sides
        ]

    near = [reduce_plane(p, axes) for p, (_, axes) in zip(products(activations, beside), sides)]
    got, across = lax.optimization_barrier((got, across))
    kept = lax.dynamic_index_in_dim(got, xh, 1, keepdims=False)
    passed = shift(lax.dynamic_index_in_dim(got, 1 - xh, 1, keepdims=False), "xh", 1)
    by_column = jnp.stack([jnp.where(xh == 0, kept, passed), jnp.where(xh == 0, passed, kept)])
    states = jnp.transpose(by_column, (2, 4, 0, 1, 3)).reshape(3, ROWS, COLS)

    far = [reduce_plane(p, axes) for p, (_, axes) in zip(products(across, shift(across, "c", 1)), sides)]

    out = jnp.zeros((2, 4, 4, ROWS, COLS), jnp.bfloat16)
    updated = []
    for (start, axes), a, b in zip(sides, near, far):
        from_a = lax.ppermute(bf16(a), ("xh", "xl"), [(2, 0), (1, 3)])
        from_b = lax.ppermute(bf16(b), ("xh", "xl"), [(0, 2), (3, 1)])
        gradient = jnp.where(xh == xl, a + f32(from_a), b + f32(from_b))
        old = f32(states[:, :, start : start + half])
        new = adam_update(old[0], old[1], old[2], gradient)
        updated.append(new)
        block = bf16(new[0])
        out = gather_plane(out, block, axes[::-1], xh, start)
        out = gather_plane(out, shift(block, "xh", 1), axes[::-1], 1 - xh, start)
    weights_new, first_new, second_new = (jnp.concatenate(pair, axis=1) for pair in zip(*updated))
    return (weights_new, first_new, second_new, out.reshape(D, COLS))


def solution(mesh):
    wide = Mesh(mesh.devices.reshape(2, 4, 4, 2, 2), ("xh", "z", "y", "xl", "c"))
    tensor = ("xl", "c")
    columns = P(None, (*tensor, *FSDP))
    rows = P(FSDP, tensor)
    return jax.shard_map(
        body,
        mesh=wide,
        in_specs=(rows, rows, columns, columns, columns),
        out_specs=(rows, rows, rows, P(None, tensor)),
        check_vma=False,
    )
```

```python
import functools

import jax
import jax.numpy as jnp
from jax import lax
from jax.experimental import pallas as pl
from jax.experimental.pallas import tpu as pltpu
from jax.sharding import Mesh, PartitionSpec as P

STEP = 20


beta_one = 0.9
beta_two = 0.95
adam_eps = 1e-08
learn_rate = 0.0003
decay_rate = 0.1

D = 5120
ROWS = 160
COLS = 1280
SIDE = 640
FSDP = ("xh", "z", "y")
SIDES = (("y", "z"), ("z", "y"))
VMEM_LIMIT = 12 * 1024 * 1024

XH, Z, Y, XL, CORE = range(5)


def f32(value):
    return value.astype(jnp.float32)


def bf16(value):
    return value.astype(jnp.bfloat16)


def shift(value, axis, step):
    count = lax.axis_size(axis)
    return lax.ppermute(value, axis, [(i, (i + step) % count) for i in range(count)])


def shape(*dims, dtype=jnp.bfloat16):
    return jax.ShapeDtypeStruct(dims, dtype)


def call(kernel, place, args, outs, scratch=(), out_space=pltpu.VMEM, aliased=0):
    vmem = pl.BlockSpec(memory_space=pltpu.VMEM)
    there = pl.BlockSpec(memory_space=out_space)
    held = len(args) - aliased
    return pl.pallas_call(
        kernel,
        out_shape=outs,
        in_specs=[pl.BlockSpec(memory_space=pltpu.SMEM)] + [vmem] * held + [there] * aliased,
        out_specs=[there] * len(outs),
        scratch_shapes=scratch,
        input_output_aliases={1 + held + i: i for i in range(aliased)},
        compiler_params=pltpu.CompilerParams(vmem_limit_bytes=VMEM_LIMIT),
    )(place, *args)


def in_rows(step):
    def run(i, carry):
        step(pl.ds(pl.multiple_of(i * 32, 32), 32))
        return carry

    lax.fori_loop(0, ROWS // 32, run, 0)


def product_kernel(place, mine, other, cotangent, *refs):
    left, right, (blocks,) = refs[:7], refs[7:14], refs[14:]
    y = place[Y]

    def y_block(steps):
        return blocks[lax.rem(y + steps, 4), :, :SIDE]

    for features, core in ((mine, place[CORE]), (other, 1 - place[CORE])):
        for low_z in range(2):
            z_of = 2 * core + low_z
            ahead = lax.rem(z_of + 4 - place[Z], 4)
            for start in (0, SIDE):
                result = lax.dot_general(
                    features[:, low_z * SIDE : (low_z + 1) * SIDE],
                    cotangent[:, start : start + SIDE],
                    (((0,), (0,)), ((), ())),
                    preferred_element_type=jnp.float32,
                )
                for j in range(4):
                    blocks[j, :, start : start + SIDE] = bf16(result[j * ROWS : (j + 1) * ROWS])

            own, far_up, far_down, near_up, near_down, hold_up, hold_down = left
            own[z_of] = y_block(0)

            @pl.when(core == 0)
            def _():
                far_up[low_z] = y_block(2)
                near_down[low_z] = y_block(3)
                hold_up[low_z] = y_block(1)

            @pl.when(core == 1)
            def _():
                near_up[low_z] = y_block(1)
                far_down[low_z] = y_block(2)
                hold_down[low_z] = y_block(3)

            own, far_up, far_down, near_up, near_down, hold_up, hold_down = right

            @pl.when(ahead == 0)
            def _():
                own[...] = blocks[:, :, SIDE:]

            for steps, low, high in ((1, hold_up, near_up), (2, far_up, far_down), (3, near_down, hold_down)):

                @pl.when(ahead == steps)
                def _():
                    low[...] = blocks[:2, :, SIDE:]
                    high[...] = blocks[2:, :, SIDE:]


def products(place, mine, other, cotangent):
    counts = (4, 2, 2, 2, 2, 2, 2) * 2
    outs = call(
        product_kernel,
        place,
        (mine, other, cotangent),
        [shape(n, ROWS, SIDE) for n in counts],
        [pltpu.VMEM((4, ROWS, COLS), jnp.bfloat16)],
    )
    return outs[:7], outs[7:]


def add_kernel(place, *refs):
    def step(rows):
        for k in range(4):
            for j in range(2):
                refs[8 + k][j, rows] = bf16(f32(refs[2 * k][j, rows]) + f32(refs[2 * k + 1][j, rows]))

    in_rows(step)


def pass_on(place, pairs):
    return call(add_kernel, place, [a for pair in pairs for a in pair], [shape(2, ROWS, SIDE)] * 4)


def finish_kernel(place, *refs):
    def step(rows):
        for s, spot in enumerate((Z, Y)):
            own, near_down, last_up, near_up, last_down = refs[5 * s : 5 * s + 5]
            outs = refs[10 + 4 * s : 14 + 4 * s]
            for steps in range(4):
                to = lax.rem(place[spot] + steps, 4)
                first, second = jnp.minimum(to, 1), jnp.maximum(to - 2, 0)
                near = jnp.where(to < 2, f32(near_down[first, rows]), f32(near_up[second, rows]))
                last = jnp.where(to < 2, f32(last_up[first, rows]), f32(last_down[second, rows]))
                value = f32(own[to, rows]) + near + last
                outs[steps][rows] = value.astype(outs[steps].dtype)

    in_rows(step)


def finish(place, sides):
    kinds = [jnp.float32, jnp.bfloat16, jnp.bfloat16, jnp.bfloat16] * 2
    outs = call(
        finish_kernel, place, [a for side in sides for a in side], [shape(ROWS, SIDE, dtype=k) for k in kinds]
    )
    return outs[:4], outs[4:]


def total_kernel(place, *refs):
    def step(rows):
        for s in range(2):
            keep, one, two, three = refs[4 * s : 4 * s + 4]
            refs[8][rows, s * SIDE : (s + 1) * SIDE] = bf16(keep[rows] + f32(one[rows]) + f32(two[rows]) + f32(three[rows]))

    in_rows(step)


def total(place, parts):
    return call(total_kernel, place, parts, [shape(ROWS, COLS)])[0]


def reduced(place, mine, other, cotangent):
    messages = products(place, mine, other, cotangent)
    far, near = [], []
    for (axis, _), m in zip(SIDES, messages):
        far.append((shift(m[1], axis, 1), shift(m[2], axis, -1)))
    for (axis, _), m in zip(SIDES, messages):
        near.append((shift(m[3], axis, 1), shift(m[4], axis, -1)))
    last = pass_on(place, [(m[5 + k], f[k]) for m, f in zip(messages, far) for k in range(2)])
    sides = []
    for s, ((axis, _), m) in enumerate(zip(SIDES, messages)):
        last_up, last_down = shift(last[2 * s], axis, 1), shift(last[2 * s + 1], axis, -1)
        sides.append((m[0], near[s][1], last_up, near[s][0], last_down))
    parts = []
    ends = finish(place, sides)
    for (_, axis), (keep, *sent) in zip(SIDES, ends):
        parts += [keep, *(shift(block, axis, k + 1) for k, block in enumerate(sent))]
    return total(place, parts), ends[0][1]


def adam_update(weights, first_moment, second_moment, gradient):
    first_new = beta_one * first_moment + (1.0 - beta_one) * gradient
    second_new = beta_two * second_moment + (1.0 - beta_two) * gradient * gradient
    corrected = first_new / (1.0 - beta_one**STEP)
    scaled = jnp.sqrt(second_new / (1.0 - beta_two**STEP)) + adam_eps
    weights_new = weights - learn_rate * (corrected / scaled + decay_rate * weights)
    return (weights_new, first_new, second_new)


def adam_kernel(place, near, near_got, far, far_got, here, there, weights, first, second, left, right):
    def step(rows):
        for half in range(2):
            is_near = half == place[XL]
            gradient = f32(jnp.where(is_near, f32(near[rows]), f32(far[rows]))) + jnp.where(
                is_near, f32(near_got[rows]), f32(far_got[rows])
            )
            for s, side in enumerate((left, right)):
                old = [
                    jnp.where(place[XH] == s, f32(here[half, k, rows]), f32(there[half, k, rows])) for k in range(3)
                ]
                columns = slice(s * SIDE, (s + 1) * SIDE)
                new = adam_update(*old, gradient[:, columns])
                side[half, rows] = bf16(new[0])

                @pl.when(half == place[XH])
                def _():
                    for ref, value in zip((weights, first, second), new):
                        ref[rows, columns] = value

    in_rows(step)


def adam(place, gradients, here, there):
    return call(
        adam_kernel,
        place,
        (*gradients, here, there),
        [shape(ROWS, COLS, dtype=jnp.float32)] * 3 + [shape(2, ROWS, SIDE)] * 2,
    )


def line_kernel(place, *refs):
    for s, spot in enumerate((Z, Y)):
        low, high = refs[8 + 2 * s], refs[9 + 2 * s]
        for k in range(4):
            block = refs[4 * s + k]
            source = lax.rem(place[spot] + 4 - k, 4)

            @pl.when(source < 2)
            def _(block=block, source=source, low=low):
                for x in range(2):
                    low[x, source] = block[x]

            @pl.when(source >= 2)
            def _(block=block, source=source, high=high):
                for x in range(2):
                    high[x, source - 2] = block[x]


def line(place, blocks):
    outs = call(line_kernel, place, blocks, [shape(2, 2, ROWS, SIDE)] * 4)
    return outs[:2], outs[2:]


def lay_kernel(steps, place, *refs):
    out, sems = refs[-2], refs[-1]
    copies = []
    for s, spot in enumerate((Y, Z)):
        columns = pl.ds(s * SIDE, SIDE)
        for k, (half, ahead) in enumerate(steps):
            other, pair = lax.rem(place[spot] + ahead, 4), pl.ds(2 * half, 2)
            index = (slice(None), pair, other) if s == 0 else (slice(None), other, pair)
            number = s * len(steps) + k
            copies.append(
                pltpu.make_async_copy(refs[number], out.at[(*index, slice(None), columns)], sems.at[number])
            )
    for copy in copies:
        copy.start()
    for copy in copies:
        copy.wait()


def lay(place, steps, pieces, *out):
    return call(
        functools.partial(lay_kernel, steps),
        place,
        [*pieces, *out],
        [shape(2, 4, 4, ROWS, COLS)],
        [pltpu.SemaphoreType.DMA((len(pieces),))],
        pltpu.HBM,
        len(out),
    )[0]


def gathered(place, blocks):
    pieces = []
    for (_, axis), block in zip(SIDES, blocks):
        pieces += [block, *(shift(block, axis, k) for k in (1, 2, 3))]
    lines = line(place, pieces)
    first = [(shift(low, axis, 1), shift(high, axis, -1)) for (axis, _), (low, high) in zip(SIDES, lines)]
    second = [(shift(high, axis, 1), shift(low, axis, -1)) for (axis, _), (low, high) in zip(SIDES, lines)]
    far = [(shift(up, axis, 1), shift(down, axis, -1)) for (axis, _), (up, down) in zip(SIDES, first)]
    near = [piece for own, a, b in zip(lines, first, second) for piece in (*own, *a, *b)]
    out = lay(place, ((0, 0), (1, 0), (0, 3), (1, 1), (1, 3), (0, 1)), near)
    return lay(place, ((0, 2), (1, 2)), [piece for pair in far for piece in pair], out)


def moved_state(states):
    flat = jnp.concatenate([bf16(s.T).reshape(40, 2, 16, ROWS) for s in states], axis=-1)
    got = lax.all_to_all(jnp.transpose(flat, (2, 1, 0, 3)), ("z", "y"), 0, 0, tiled=True)
    return jnp.transpose(got, (1, 3, 0, 2)).reshape(2, 3, ROWS, SIDE)


def body(activations, cotangent, weights, first_moment, second_moment):
    place = jnp.stack([lax.axis_index(a) for a in ("xh", "z", "y", "xl", "c")]).astype(jnp.int32)
    across = shift(activations, "xl", 1)
    beside = shift(activations, "c", 1)
    near, sent = reduced(place, activations, beside, cotangent)
    here = moved_state((weights, first_moment, second_moment))
    across, _ = lax.optimization_barrier((across, sent))
    far, _ = reduced(place, across, shift(across, "c", 1), cotangent)
    _, here, near = lax.optimization_barrier((across, here, near))
    near_got = shift(near, "xh", 1)
    there = shift(here, "xh", 1)
    far_got = shift(far, "xh", 1)
    weights_new, first_new, second_new, left, right = adam(place, (near, near_got, far, far_got), here, there)
    out = gathered(place, (left, right))
    return (weights_new, first_new, second_new, out.reshape(D, COLS))


def solution(mesh):
    wide = Mesh(mesh.devices.reshape(2, 4, 4, 2, 2), ("xh", "z", "y", "xl", "c"))
    tensor = ("xl", "c")
    columns = P(None, (*tensor, *FSDP))
    rows = P(FSDP, tensor)
    return jax.shard_map(
        body,
        mesh=wide,
        in_specs=(rows, rows, columns, columns, columns),
        out_specs=(rows, rows, rows, P(None, tensor)),
        check_vma=False,
    )
```

```python
import functools

import jax
import jax.numpy as jnp
from jax import lax
from jax.experimental import pallas as pl
from jax.experimental.pallas import tpu as pltpu
from jax.sharding import Mesh, PartitionSpec as P

STEP = 20


beta_one = 0.9
beta_two = 0.95
adam_eps = 1e-08
learn_rate = 0.0003
decay_rate = 0.1

D = 5120
ROWS = 160
COLS = 1280
SIDE = 640
FSDP = ("xh", "z", "y")
SIDES = (("y", "z"), ("z", "y"))
VMEM_LIMIT = 12 * 1024 * 1024

XH, Z, Y, XL, CORE = range(5)


def f32(value):
    return value.astype(jnp.float32)


def bf16(value):
    return value.astype(jnp.bfloat16)


def shift(value, axis, step):
    count = lax.axis_size(axis)
    return lax.ppermute(value, axis, [(i, (i + step) % count) for i in range(count)])


def shape(*dims, dtype=jnp.bfloat16):
    return jax.ShapeDtypeStruct(dims, dtype)


def call(kernel, place, args, outs, scratch=(), out_space=pltpu.VMEM, aliased=0):
    vmem = pl.BlockSpec(memory_space=pltpu.VMEM)
    there = pl.BlockSpec(memory_space=out_space)
    held = len(args) - aliased
    return pl.pallas_call(
        kernel,
        out_shape=outs,
        in_specs=[pl.BlockSpec(memory_space=pltpu.SMEM)] + [vmem] * held + [there] * aliased,
        out_specs=[there] * len(outs),
        scratch_shapes=scratch,
        input_output_aliases={1 + held + i: i for i in range(aliased)},
        compiler_params=pltpu.CompilerParams(vmem_limit_bytes=VMEM_LIMIT),
    )(place, *args)


def in_rows(step):
    def run(i, carry):
        step(pl.ds(pl.multiple_of(i * 32, 32), 32))
        return carry

    lax.fori_loop(0, ROWS // 32, run, 0)


def multiply(features, cotangent, blocks):
    def one(low_z, carry):
        result = lax.dot_general(
            features[:, pl.ds(pl.multiple_of(low_z * SIDE, 128), SIDE)],
            cotangent[...],
            (((0,), (0,)), ((), ())),
            preferred_element_type=jnp.float32,
        )
        for s in range(2):
            for j in range(4):
                blocks[low_z, s, j] = bf16(result[j * ROWS : (j + 1) * ROWS, s * SIDE : (s + 1) * SIDE])
        return carry

    lax.fori_loop(0, 2, one, 0)


def first_product_kernel(place, features, cotangent, made):
    multiply(features, cotangent, made)


def product_kernel(place, made, features, cotangent, *refs):
    left, right, blocks = refs[:7], refs[7:14], refs[14]
    multiply(features, cotangent, blocks)

    def arrange(values, core, low_z):
        z_of = 2 * core + low_z
        ahead = lax.rem(z_of + 4 - place[Z], 4)

        def y_block(steps):
            return values[low_z, 0, lax.rem(place[Y] + steps, 4)]

        own, far_up, far_down, near_up, near_down, hold_up, hold_down = left
        own[z_of] = y_block(0)

        @pl.when(core == 0)
        def _():
            far_up[low_z] = y_block(2)
            near_down[low_z] = y_block(3)
            hold_up[low_z] = y_block(1)

        @pl.when(core == 1)
        def _():
            near_up[low_z] = y_block(1)
            far_down[low_z] = y_block(2)
            hold_down[low_z] = y_block(3)

        own, far_up, far_down, near_up, near_down, hold_up, hold_down = right

        @pl.when(ahead == 0)
        def _():
            own[...] = values[low_z, 1]

        for steps, low, high in ((1, hold_up, near_up), (2, far_up, far_down), (3, near_down, hold_down)):

            @pl.when(ahead == steps)
            def _():
                low[...] = values[low_z, 1, :2]
                high[...] = values[low_z, 1, 2:]

    def one(low_z, carry):
        arrange(made, place[CORE], low_z)
        arrange(blocks, 1 - place[CORE], low_z)
        return carry

    lax.fori_loop(0, 2, one, 0)


def products(place, cotangent, mine, other):
    made = call(first_product_kernel, place, (mine, cotangent), [shape(2, 2, 4, ROWS, SIDE)])[0]
    outs = call(
        product_kernel,
        place,
        (made, other, cotangent),
        [shape(n, ROWS, SIDE) for n in (4, 2, 2, 2, 2, 2, 2) * 2],
        [pltpu.VMEM((2, 2, 4, ROWS, SIDE), jnp.bfloat16)],
    )
    return outs[:7], outs[7:]


def add_kernel(place, *refs):
    def step(rows):
        for k in range(4):
            for j in range(2):
                refs[8 + k][j, rows] = bf16(f32(refs[2 * k][j, rows]) + f32(refs[2 * k + 1][j, rows]))

    in_rows(step)


def pass_on(place, pairs):
    return call(add_kernel, place, [a for pair in pairs for a in pair], [shape(2, ROWS, SIDE)] * 4)


def finish_kernel(place, *refs):
    def step(rows):
        for s, spot in enumerate((Z, Y)):
            own, near_down, last_up, near_up, last_down = refs[5 * s : 5 * s + 5]
            outs = refs[10 + 4 * s : 14 + 4 * s]
            for steps in range(4):
                to = lax.rem(place[spot] + steps, 4)
                first, second = jnp.minimum(to, 1), jnp.maximum(to - 2, 0)
                near = jnp.where(to < 2, f32(near_down[first, rows]), f32(near_up[second, rows]))
                last = jnp.where(to < 2, f32(last_up[first, rows]), f32(last_down[second, rows]))
                value = f32(own[to, rows]) + near + last
                outs[steps][rows] = value.astype(outs[steps].dtype)

    in_rows(step)


def finish(place, sides):
    kinds = [jnp.float32, jnp.bfloat16, jnp.bfloat16, jnp.bfloat16] * 2
    outs = call(
        finish_kernel, place, [a for side in sides for a in side], [shape(ROWS, SIDE, dtype=k) for k in kinds]
    )
    return outs[:4], outs[4:]


def total_kernel(place, *refs):
    def step(rows):
        for s in range(2):
            keep, one, two, three = refs[4 * s : 4 * s + 4]
            refs[8][rows, s * SIDE : (s + 1) * SIDE] = bf16(keep[rows] + f32(one[rows]) + f32(two[rows]) + f32(three[rows]))

    in_rows(step)


def total(place, parts):
    return call(total_kernel, place, parts, [shape(ROWS, COLS)])[0]


def reduced(place, messages):
    far, near = [], []
    for (axis, _), m in zip(SIDES, messages):
        far.append((shift(m[1], axis, 1), shift(m[2], axis, -1)))
    for (axis, _), m in zip(SIDES, messages):
        near.append((shift(m[3], axis, 1), shift(m[4], axis, -1)))
    last = pass_on(place, [(m[5 + k], f[k]) for m, f in zip(messages, far) for k in range(2)])
    sides = []
    for s, ((axis, _), m) in enumerate(zip(SIDES, messages)):
        last_up, last_down = shift(last[2 * s], axis, 1), shift(last[2 * s + 1], axis, -1)
        sides.append((m[0], near[s][1], last_up, near[s][0], last_down))
    parts = []
    ends = finish(place, sides)
    for (_, axis), (keep, *sent) in zip(SIDES, ends):
        parts += [keep, *(shift(block, axis, k + 1) for k, block in enumerate(sent))]
    return total(place, parts), ends[0][1]


def adam_update(weights, first_moment, second_moment, gradient):
    first_new = beta_one * first_moment + (1.0 - beta_one) * gradient
    second_new = beta_two * second_moment + (1.0 - beta_two) * gradient * gradient
    corrected = first_new / (1.0 - beta_one**STEP)
    scaled = jnp.sqrt(second_new / (1.0 - beta_two**STEP)) + adam_eps
    weights_new = weights - learn_rate * (corrected / scaled + decay_rate * weights)
    return (weights_new, first_new, second_new)


def adam_kernel(place, near, near_got, far, far_got, here, there, weights, first, second, left, right):
    def step(rows):
        for half in range(2):
            is_near = half == place[XL]
            gradient = f32(jnp.where(is_near, f32(near[rows]), f32(far[rows]))) + jnp.where(
                is_near, f32(near_got[rows]), f32(far_got[rows])
            )
            for s, side in enumerate((left, right)):
                old = [
                    jnp.where(place[XH] == s, f32(here[half, k, rows]), f32(there[half, k, rows])) for k in range(3)
                ]
                columns = slice(s * SIDE, (s + 1) * SIDE)
                new = adam_update(*old, gradient[:, columns])
                side[half, rows] = bf16(new[0])

                @pl.when(half == place[XH])
                def _():
                    for ref, value in zip((weights, first, second), new):
                        ref[rows, columns] = value

    in_rows(step)


def adam(place, gradients, here, there):
    return call(
        adam_kernel,
        place,
        (*gradients, here, there),
        [shape(ROWS, COLS, dtype=jnp.float32)] * 3 + [shape(2, ROWS, SIDE)] * 2,
    )


def line_kernel(place, *refs):
    for s, spot in enumerate((Z, Y)):
        low, high = refs[8 + 2 * s], refs[9 + 2 * s]
        for k in range(4):
            block = refs[4 * s + k]
            source = lax.rem(place[spot] + 4 - k, 4)

            @pl.when(source < 2)
            def _(block=block, source=source, low=low):
                for x in range(2):
                    low[x, source] = block[x]

            @pl.when(source >= 2)
            def _(block=block, source=source, high=high):
                for x in range(2):
                    high[x, source - 2] = block[x]


def line(place, blocks):
    outs = call(line_kernel, place, blocks, [shape(2, 2, ROWS, SIDE)] * 4)
    return outs[:2], outs[2:]


def lay_kernel(steps, place, *refs):
    out, sems = refs[-2], refs[-1]
    copies = []
    for s, spot in enumerate((Y, Z)):
        columns = pl.ds(s * SIDE, SIDE)
        for k, (half, ahead) in enumerate(steps):
            other, pair = lax.rem(place[spot] + ahead, 4), pl.ds(2 * half, 2)
            index = (slice(None), pair, other) if s == 0 else (slice(None), other, pair)
            number = s * len(steps) + k
            copies.append(
                pltpu.make_async_copy(refs[number], out.at[(*index, slice(None), columns)], sems.at[number])
            )
    for copy in copies:
        copy.start()
    for copy in copies:
        copy.wait()


def lay(place, steps, pieces, *out):
    return call(
        functools.partial(lay_kernel, steps),
        place,
        [*pieces, *out],
        [shape(2, 4, 4, ROWS, COLS)],
        [pltpu.SemaphoreType.DMA((len(pieces),))],
        pltpu.HBM,
        len(out),
    )[0]


def gathered(place, blocks):
    pieces = []
    for (_, axis), block in zip(SIDES, blocks):
        pieces += [block, *(shift(block, axis, k) for k in (1, 2, 3))]
    lines = line(place, pieces)
    first = [(shift(low, axis, 1), shift(high, axis, -1)) for (axis, _), (low, high) in zip(SIDES, lines)]
    second = [(shift(high, axis, 1), shift(low, axis, -1)) for (axis, _), (low, high) in zip(SIDES, lines)]
    far = [(shift(up, axis, 1), shift(down, axis, -1)) for (axis, _), (up, down) in zip(SIDES, first)]
    near = [piece for own, a, b in zip(lines, first, second) for piece in (*own, *a, *b)]
    out = lay(place, ((0, 0), (1, 0), (0, 3), (1, 1), (1, 3), (0, 1)), near)
    return lay(place, ((0, 2), (1, 2)), [piece for pair in far for piece in pair], out)


def state_kernel(place, got, out, turned):
    def half(h, carry):
        for source in range(16):
            turned[source * 40 : (source + 1) * 40, :480] = f32(got[source, h])
        flat = turned[...].T
        for k in range(3):
            out[h, k] = bf16(flat[k * ROWS : (k + 1) * ROWS])
        return carry

    turned[:, 480:] = jnp.zeros((SIDE, 32), jnp.float32)
    lax.fori_loop(0, 2, half, 0)


def send_kernel(place, *refs):
    states, out = refs[:3], refs[3]

    def four(g, carry):
        for j in range(4):
            block = 4 * g + j
            for k, state in enumerate(states):
                rows = state[:, pl.ds(pl.multiple_of(g * SIDE, 128), SIDE)]
                out[lax.rem(block, 16), lax.div(block, 16), :, k * ROWS : (k + 1) * ROWS] = bf16(
                    rows[:, j * ROWS : (j + 1) * ROWS]
                )
        return carry

    lax.fori_loop(0, 8, four, 0)


def sent_state(place, states):
    return call(send_kernel, place, [s.T for s in states], [shape(16, 2, 40, 3 * ROWS)])[0]


def moved_state(place, flat):
    got = lax.all_to_all(flat, ("z", "y"), 0, 0, tiled=True)
    return call(
        state_kernel, place, (got,), [shape(2, 3, ROWS, SIDE)], [pltpu.VMEM((SIDE, 512), jnp.float32)]
    )[0]


def step(activations, cotangent, weights, first_moment, second_moment):
    place = jnp.stack([lax.axis_index(a) for a in ("xh", "z", "y", "xl", "c")]).astype(jnp.int32)
    across = shift(activations, "xl", 1)
    beside = shift(activations, "c", 1)
    flat = sent_state(place, (weights, first_moment, second_moment))
    beside, flat = lax.optimization_barrier((beside, flat))
    messages = products(place, cotangent, activations, beside)
    here = moved_state(place, flat)
    near, sent = reduced(place, messages)

    across, here, _ = lax.optimization_barrier((across, here, sent))
    there = shift(here, "xh", 1)
    messages = products(place, cotangent, across, shift(across, "c", 1))
    far, _ = reduced(place, messages)
    near_got = shift(near, "xh", 1)
    far_got = shift(far, "xh", 1)
    weights_new, first_new, second_new, left, right = adam(place, (near, near_got, far, far_got), here, there)
    out = gathered(place, (left, right))
    return (weights_new, first_new, second_new, out.reshape(D, COLS))


def solution(mesh):
    wide = Mesh(mesh.devices.reshape(2, 4, 4, 2, 2), ("xh", "z", "y", "xl", "c"))
    tensor = ("xl", "c")
    columns = P(None, (*tensor, *FSDP))
    rows = P(FSDP, tensor)
    return jax.shard_map(
        step,
        mesh=wide,
        in_specs=(rows, rows, columns, columns, columns),
        out_specs=(rows, rows, rows, P(None, tensor)),
        check_vma=False,
    )
```

```python
import functools

import jax
import jax.numpy as jnp
from jax import lax
from jax.experimental import pallas as pl
from jax.experimental.pallas import tpu as pltpu
from jax.sharding import Mesh, PartitionSpec as P

STEP = 20


beta_one = 0.9
beta_two = 0.95
adam_eps = 1e-08
learn_rate = 0.0003
decay_rate = 0.1

D = 5120
ROWS = 160
COLS = 1280
PART = 640
FSDP = ("xh", "z", "y")
VMEM_LIMIT = 12 * 1024 * 1024

XH, Z, Y, XL, CORE, FIRST, SECOND = range(7)


def f32(value):
    return value.astype(jnp.float32)


def bf16(value):
    return value.astype(jnp.bfloat16)


def shift(value, axis, step):
    count = lax.axis_size(axis)
    return lax.ppermute(value, axis, [(i, (i + step) % count) for i in range(count)])


def ring(value, second, step):
    pairs = []
    for z in range(4):
        for y in range(4):
            for core in range(2):
                along_y = core == second
                to = (z, (y + step) % 4) if along_y else ((z + step) % 4, y)
                pairs.append(((z * 4 + y) * 2 + core, (to[0] * 4 + to[1]) * 2 + core))
    return lax.ppermute(value, ("z", "y", "c"), pairs)


def shape(*dims, dtype=jnp.bfloat16):
    return jax.ShapeDtypeStruct(dims, dtype)


def call(kernel, place, args, outs, scratch=(), out_spaces=None, aliased=0):
    vmem = pl.BlockSpec(memory_space=pltpu.VMEM)
    there = [pl.BlockSpec(memory_space=space) for space in out_spaces or (pltpu.VMEM,) * len(outs)]
    held = len(args) - aliased
    return pl.pallas_call(
        kernel,
        out_shape=outs,
        in_specs=[pl.BlockSpec(memory_space=pltpu.SMEM)] + [vmem] * held + there[:aliased],
        out_specs=there,
        scratch_shapes=scratch,
        input_output_aliases={1 + held + i: i for i in range(aliased)},
        compiler_params=pltpu.CompilerParams(vmem_limit_bytes=VMEM_LIMIT),
    )(place, *args)


def in_rows(step):
    def run(i, carry):
        step(pl.ds(pl.multiple_of(i * 32, 32), 32))
        return carry

    lax.fori_loop(0, ROWS // 32, run, 0)


def multiply(features, cotangent, blocks):
    def one(low_z, carry):
        result = lax.dot_general(
            features[:, pl.ds(pl.multiple_of(low_z * 640, 128), 640)],
            cotangent[...],
            (((0,), (0,)), ((), ())),
            preferred_element_type=jnp.float32,
        )
        for j in range(4):
            blocks[low_z, j] = bf16(result[j * ROWS : (j + 1) * ROWS])
        return carry

    lax.fori_loop(0, 2, one, 0)


def first_product_kernel(place, features, cotangent, made):
    multiply(features, cotangent, made)


def product_kernel(place, made, features, cotangent, *refs):
    far_up, far_down, hold_up, hold_down, own, near_up, near_down, blocks, sems = refs
    multiply(features, cotangent, blocks)

    def send(value, ref, k):
        pltpu.make_async_copy(value, ref, sems.at[k]).start()

    def over_y(values, owner, low_z):
        def y_block(steps):
            return values.at[low_z, lax.rem(place[Y] + steps, 4)]

        send(y_block(0), own.at[2 * owner + low_z], 0)
        if owner == 0:
            send(y_block(3), near_down.at[low_z], 2)
            far_up[low_z] = y_block(2)[...]
            hold_up[low_z] = y_block(1)[...]
        else:
            send(y_block(1), near_up.at[low_z], 1)
            far_down[low_z] = y_block(2)[...]
            hold_down[low_z] = y_block(3)[...]

    def over_z(values, owner, low_z):
        ahead = lax.rem(2 * owner + low_z + 4 - place[Z], 4)

        @pl.when(ahead == 0)
        def _():
            send(values.at[low_z], own, 0)

        @pl.when(ahead == 1)
        def _():
            send(values.at[low_z, pl.ds(2, 2)], near_up, 1)
            hold_up[...] = values[low_z, :2]

        @pl.when(ahead == 2)
        def _():
            far_up[...] = values[low_z, :2]
            far_down[...] = values[low_z, 2:]

        @pl.when(ahead == 3)
        def _():
            send(values.at[low_z, pl.ds(0, 2)], near_down, 2)
            hold_down[...] = values[low_z, 2:]

    for core, arrange in ((0, over_y), (1, over_z)):

        @pl.when(place[CORE] == core)
        def _():
            for low_z in range(2):
                arrange(made, core, low_z)
                arrange(blocks, 1 - core, low_z)

    pltpu.make_async_copy(blocks.at[0], own, sems.at[0]).wait()
    pltpu.make_async_copy(blocks.at[0, pl.ds(0, 2)], near_up, sems.at[1]).wait()
    pltpu.make_async_copy(blocks.at[0, pl.ds(0, 2)], near_down, sems.at[2]).wait()


def products(place, cotangent, mine, other):
    made = call(first_product_kernel, place, (mine, cotangent), [shape(2, 4, ROWS, COLS)])[0]
    return call(
        product_kernel,
        place,
        (made, other, cotangent),
        [shape(n, ROWS, COLS) for n in (2, 2, 2, 2, 4, 2, 2)],
        [pltpu.VMEM((2, 4, ROWS, COLS), jnp.bfloat16), pltpu.SemaphoreType.DMA((3,))],
        (pltpu.VMEM,) * 4 + (pltpu.HBM,) * 3,
    )


def add_kernel(place, *refs):
    def step(rows):
        for k in range(2):
            for j in range(2):
                refs[4 + k][j, rows] = bf16(f32(refs[2 * k][j, rows]) + f32(refs[2 * k + 1][j, rows]))

    in_rows(step)


def pass_on(place, *blocks):
    return call(add_kernel, place, blocks, [shape(2, ROWS, COLS)] * 2)


def finish_kernel(place, own, near_down, last_up, near_up, last_down, *outs):
    def step(rows):
        for steps in range(4):
            to = lax.rem(place[SECOND] + steps, 4)
            first, second = jnp.minimum(to, 1), jnp.maximum(to - 2, 0)
            near = jnp.where(to < 2, f32(near_down[first, rows]), f32(near_up[second, rows]))
            last = jnp.where(to < 2, f32(last_up[first, rows]), f32(last_down[second, rows]))
            value = f32(own[to, rows]) + near + last
            outs[steps][rows] = value.astype(outs[steps].dtype)

    in_rows(step)


def finish(place, *blocks):
    kinds = (jnp.float32, jnp.bfloat16, jnp.bfloat16, jnp.bfloat16)
    return call(finish_kernel, place, blocks, [shape(ROWS, COLS, dtype=k) for k in kinds])


def total_kernel(place, keep, one, two, three, out):
    def step(rows):
        out[rows] = bf16(keep[rows] + f32(one[rows]) + f32(two[rows]) + f32(three[rows]))

    in_rows(step)


def reduced(place, messages):
    far_up, far_down, hold_up, hold_down, own, near_up, near_down = messages
    far_up, far_down = ring(far_up, 0, 1), ring(far_down, 0, -1)
    near_up, near_down = ring(near_up, 0, 1), ring(near_down, 0, -1)
    last_up, last_down = pass_on(place, hold_up, far_up, hold_down, far_down)
    last_up, last_down = ring(last_up, 0, 1), ring(last_down, 0, -1)
    keep, *sent = finish(place, own, near_down, last_up, near_up, last_down)
    got = [ring(block, 1, k + 1) for k, block in enumerate(sent)]
    return call(total_kernel, place, (keep, *got), [shape(ROWS, COLS)])[0], sent[0]


def adam_update(weights, first_moment, second_moment, gradient):
    first_new = beta_one * first_moment + (1.0 - beta_one) * gradient
    second_new = beta_two * second_moment + (1.0 - beta_two) * gradient * gradient
    corrected = first_new * (1.0 / (1.0 - beta_one**STEP))
    scaled = jnp.sqrt(second_new * (1.0 / (1.0 - beta_two**STEP))) + adam_eps
    weights_new = weights - learn_rate * (corrected / scaled + decay_rate * weights)
    return (weights_new, first_new, second_new)


def adam_kernel(place, near, near_got, far, far_got, here, there, weights, first, second, *both):
    def step(rows):
        for half in range(2):
            is_near = half == place[XL]
            gradient = f32(jnp.where(is_near, f32(near[rows]), f32(far[rows]))) + jnp.where(
                is_near, f32(near_got[rows]), f32(far_got[rows])
            )
            for s in range(2):
                old = [
                    jnp.where(place[XH] == s, f32(here[half, k, rows]), f32(there[half, k, rows])) for k in range(3)
                ]
                columns = slice(s * PART, (s + 1) * PART)
                new = adam_update(*old, gradient[:, columns])
                both[half][rows, columns] = bf16(new[0])

                @pl.when(half == place[XH])
                def _():
                    for ref, value in zip((weights, first, second), new):
                        ref[rows, columns] = value

    in_rows(step)


def adam(place, gradients, here, there):
    return call(
        adam_kernel,
        place,
        (*gradients, here, there),
        [shape(ROWS, COLS, dtype=jnp.float32)] * 3 + [shape(ROWS, COLS)] * 2,
    )


def line_kernel(place, *refs):
    low, high = refs[8:]
    for ahead in range(4):
        source = lax.rem(place[SECOND] + ahead, 4)

        @pl.when(source < 2)
        def _():
            for x in range(2):
                low[x, source] = refs[2 * ahead + x][...]

        @pl.when(source >= 2)
        def _():
            for x in range(2):
                high[x, source - 2] = refs[2 * ahead + x][...]


def lay_kernel(steps, place, *refs):
    out, sems = refs[-2], refs[-1]

    def copy(k, along_y):
        half, ahead = steps[k]
        other, pair = lax.rem(place[FIRST] + ahead, 4), pl.ds(2 * half, 2)
        index = (slice(None), pair, other) if along_y else (slice(None), other, pair)
        return pltpu.make_async_copy(refs[k], out.at[index], sems.at[k])

    for core in range(2):

        @pl.when(place[CORE] == core)
        def _():
            for k in range(len(steps)):
                copy(k, core == 0).start()
            for k in range(len(steps)):
                copy(k, core == 0).wait()


def lay(place, steps, pieces, *out):
    return call(
        functools.partial(lay_kernel, steps),
        place,
        [*pieces, *out],
        [shape(2, 4, 4, ROWS, COLS)],
        [pltpu.SemaphoreType.DMA((len(pieces),))],
        (pltpu.HBM,),
        len(out),
    )[0]


def gather_ring(low, high, second):
    low_up, high_down = ring(low, second, 1), ring(high, second, -1)
    high_up, low_down = ring(high, second, 1), ring(low, second, -1)
    far_up, far_down = ring(low_up, second, 1), ring(high_down, second, -1)
    return low_down, high_down, far_up, far_down, low_up, high_up


def gathered(place, both):
    blocks = (*both, *gather_ring(*both, 1))
    low, high = call(line_kernel, place, blocks, [shape(2, 2, ROWS, COLS)] * 2)
    low_down, high_down, far_up, far_down, low_up, high_up = gather_ring(low, high, 0)
    steps = ((0, 0), (1, 0), (0, 3), (1, 1), (1, 3), (0, 1))
    out = lay(place, steps, (low, high, low_up, high_down, high_up, low_down))
    return lay(place, ((0, 2), (1, 2)), (far_up, far_down), out)


def state_kernel(place, got, out, turned):
    def half(h, carry):
        for source in range(16):
            turned[source * 40 : (source + 1) * 40, :480] = f32(got[source, h])
        flat = turned[...].T
        for k in range(3):
            out[h, k] = bf16(flat[k * ROWS : (k + 1) * ROWS])
        return carry

    turned[:, 480:] = jnp.zeros((PART, 32), jnp.float32)
    lax.fori_loop(0, 2, half, 0)


def send_kernel(place, *refs):
    states, out = refs[:3], refs[3]

    def four(g, carry):
        for j in range(4):
            block = 4 * g + j
            for k, state in enumerate(states):
                rows = state[:, pl.ds(pl.multiple_of(g * 640, 128), 640)]
                out[lax.rem(block, 16), lax.div(block, 16), :, k * ROWS : (k + 1) * ROWS] = bf16(
                    rows[:, j * ROWS : (j + 1) * ROWS]
                )
        return carry

    lax.fori_loop(0, 8, four, 0)


def sent_state(place, states):
    return call(send_kernel, place, [s.T for s in states], [shape(16, 2, 40, 3 * ROWS)])[0]


def moved_state(place, flat):
    got = lax.all_to_all(flat, ("z", "y"), 0, 0, tiled=True)
    return call(
        state_kernel, place, (got,), [shape(2, 3, ROWS, PART)], [pltpu.VMEM((PART, 512), jnp.float32)]
    )[0]


def step(activations, cotangent, weights, first_moment, second_moment):
    place = [lax.axis_index(a) for a in ("xh", "z", "y", "xl", "c")]
    swapped = place[CORE] == 1
    place += [jnp.where(swapped, place[Z], place[Y]), jnp.where(swapped, place[Y], place[Z])]
    place = jnp.stack(place).astype(jnp.int32)
    across = shift(activations, "xl", 1)
    beside = shift(activations, "c", 1)
    flat = sent_state(place, (weights, first_moment, second_moment))
    here = moved_state(place, flat)
    messages = products(place, cotangent, activations, beside)
    near, sent = reduced(place, messages)

    across, here, _ = lax.optimization_barrier((across, here, sent))
    there = shift(here, "xh", 1)
    messages = products(place, cotangent, across, shift(across, "c", 1))
    near_got = shift(near, "xh", 1)
    far, _ = reduced(place, messages)
    far_got = shift(far, "xh", 1)
    weights_new, first_new, second_new, *both = adam(place, (near, near_got, far, far_got), here, there)
    out = gathered(place, both)
    return (weights_new, first_new, second_new, out.reshape(D, COLS))


def solution(mesh):
    wide = Mesh(mesh.devices.reshape(2, 4, 4, 2, 2), ("xh", "z", "y", "xl", "c"))
    tensor = ("xl", "c")
    columns = P(None, (*tensor, *FSDP))
    rows = P(FSDP, tensor)
    return jax.shard_map(
        step,
        mesh=wide,
        in_specs=(rows, rows, columns, columns, columns),
        out_specs=(rows, rows, rows, P(None, tensor)),
        check_vma=False,
    )
```

```python
import functools

import jax
import jax.numpy as jnp
from jax import lax
from jax.experimental import pallas as pl
from jax.experimental.pallas import tpu as pltpu
from jax.sharding import Mesh, PartitionSpec as P

STEP = 20


beta_one = 0.9
beta_two = 0.95
adam_eps = 1e-08
learn_rate = 0.0003
decay_rate = 0.1

D = 5120
ROWS = 160
COLS = 1280
PART = 640
FSDP = ("xh", "z", "y")
VMEM_LIMIT = 12 * 1024 * 1024

XH, Z, Y, XL, CORE, FIRST, SECOND = range(7)


def f32(value):
    return value.astype(jnp.float32)


def bf16(value):
    return value.astype(jnp.bfloat16)


def shift(value, axis, step):
    count = lax.axis_size(axis)
    return lax.ppermute(value, axis, [(i, (i + step) % count) for i in range(count)])


def ring(value, second, step):
    pairs = []
    for z in range(4):
        for y in range(4):
            for core in range(2):
                along_y = core == second
                to = (z, (y + step) % 4) if along_y else ((z + step) % 4, y)
                pairs.append(((z * 4 + y) * 2 + core, (to[0] * 4 + to[1]) * 2 + core))
    return lax.ppermute(value, ("z", "y", "c"), pairs)


def shape(*dims, dtype=jnp.bfloat16):
    return jax.ShapeDtypeStruct(dims, dtype)


def call(kernel, place, args, outs, scratch=(), out_spaces=None, aliased=0):
    vmem = pl.BlockSpec(memory_space=pltpu.VMEM)
    there = [pl.BlockSpec(memory_space=space) for space in out_spaces or (pltpu.VMEM,) * len(outs)]
    held = len(args) - aliased
    return pl.pallas_call(
        kernel,
        out_shape=outs,
        in_specs=[pl.BlockSpec(memory_space=pltpu.SMEM)] + [vmem] * held + there[:aliased],
        out_specs=there,
        scratch_shapes=scratch,
        input_output_aliases={1 + held + i: i for i in range(aliased)},
        compiler_params=pltpu.CompilerParams(vmem_limit_bytes=VMEM_LIMIT),
    )(place, *args)


def in_rows(step):
    def run(i, carry):
        step(pl.ds(pl.multiple_of(i * 32, 32), 32))
        return carry

    lax.fori_loop(0, ROWS // 32, run, 0)


def multiply(features, cotangent, blocks):
    def one(low_z, carry):
        result = lax.dot_general(
            features[:, pl.ds(pl.multiple_of(low_z * 640, 128), 640)],
            cotangent[...],
            (((0,), (0,)), ((), ())),
            preferred_element_type=jnp.float32,
        )
        for j in range(4):
            blocks[low_z, j] = bf16(result[j * ROWS : (j + 1) * ROWS])
        return carry

    lax.fori_loop(0, 2, one, 0)


def first_product_kernel(place, features, cotangent, made):
    multiply(features, cotangent, made)


def product_kernel(place, made, features, cotangent, *refs):
    far_up, far_down, hold_up, hold_down, own, near_up, near_down, blocks, sems = refs
    multiply(features, cotangent, blocks)

    def send(value, ref, k):
        pltpu.make_async_copy(value, ref, sems.at[k]).start()

    def over_y(values, owner, low_z):
        def y_block(steps):
            return values.at[low_z, lax.rem(place[Y] + steps, 4)]

        send(y_block(0), own.at[2 * owner + low_z], 0)
        if owner == 0:
            send(y_block(3), near_down.at[low_z], 2)
            far_up[low_z] = y_block(2)[...]
            hold_up[low_z] = y_block(1)[...]
        else:
            send(y_block(1), near_up.at[low_z], 1)
            far_down[low_z] = y_block(2)[...]
            hold_down[low_z] = y_block(3)[...]

    def over_z(values, owner, low_z):
        ahead = lax.rem(2 * owner + low_z + 4 - place[Z], 4)

        @pl.when(ahead == 0)
        def _():
            send(values.at[low_z], own, 0)

        @pl.when(ahead == 1)
        def _():
            send(values.at[low_z, pl.ds(2, 2)], near_up, 1)
            hold_up[...] = values[low_z, :2]

        @pl.when(ahead == 2)
        def _():
            far_up[...] = values[low_z, :2]
            far_down[...] = values[low_z, 2:]

        @pl.when(ahead == 3)
        def _():
            send(values.at[low_z, pl.ds(0, 2)], near_down, 2)
            hold_down[...] = values[low_z, 2:]

    for core, arrange in ((0, over_y), (1, over_z)):

        @pl.when(place[CORE] == core)
        def _():
            for low_z in range(2):
                arrange(made, core, low_z)
                arrange(blocks, 1 - core, low_z)

    pltpu.make_async_copy(blocks.at[0], own, sems.at[0]).wait()
    pltpu.make_async_copy(blocks.at[0, pl.ds(0, 2)], near_up, sems.at[1]).wait()
    pltpu.make_async_copy(blocks.at[0, pl.ds(0, 2)], near_down, sems.at[2]).wait()


def products(place, cotangent, mine, other):
    made = call(first_product_kernel, place, (mine, cotangent), [shape(2, 4, ROWS, COLS)])[0]
    return call(
        product_kernel,
        place,
        (made, other, cotangent),
        [shape(n, ROWS, COLS) for n in (2, 2, 2, 2, 4, 2, 2)],
        [pltpu.VMEM((2, 4, ROWS, COLS), jnp.bfloat16), pltpu.SemaphoreType.DMA((3,))],
        (pltpu.VMEM,) * 4 + (pltpu.HBM,) * 3,
    )


def add_kernel(place, *refs):
    def step(rows):
        for k in range(2):
            for j in range(2):
                refs[4 + k][j, rows] = bf16(f32(refs[2 * k][j, rows]) + f32(refs[2 * k + 1][j, rows]))

    in_rows(step)


def pass_on(place, *blocks):
    return call(add_kernel, place, blocks, [shape(2, ROWS, COLS)] * 2)


def finish_kernel(place, own, near_down, last_up, near_up, last_down, *outs):
    def step(rows):
        for steps in range(4):
            to = lax.rem(place[SECOND] + steps, 4)
            first, second = jnp.minimum(to, 1), jnp.maximum(to - 2, 0)
            near = jnp.where(to < 2, f32(near_down[first, rows]), f32(near_up[second, rows]))
            last = jnp.where(to < 2, f32(last_up[first, rows]), f32(last_down[second, rows]))
            value = f32(own[to, rows]) + near + last
            outs[steps][rows] = value.astype(outs[steps].dtype)

    in_rows(step)


def finish(place, *blocks):
    kinds = (jnp.float32, jnp.bfloat16, jnp.bfloat16, jnp.bfloat16)
    return call(finish_kernel, place, blocks, [shape(ROWS, COLS, dtype=k) for k in kinds])


def total_kernel(place, keep, one, two, three, out):
    def step(rows):
        out[rows] = bf16(keep[rows] + f32(one[rows]) + f32(two[rows]) + f32(three[rows]))

    in_rows(step)


def reduced(place, messages):
    far_up, far_down, hold_up, hold_down, own, near_up, near_down = messages
    far_up, far_down = ring(far_up, 0, 1), ring(far_down, 0, -1)
    near_up, near_down = ring(near_up, 0, 1), ring(near_down, 0, -1)
    last_up, last_down = pass_on(place, hold_up, far_up, hold_down, far_down)
    last_up, last_down = ring(last_up, 0, 1), ring(last_down, 0, -1)
    keep, *sent = finish(place, own, near_down, last_up, near_up, last_down)
    got = [ring(block, 1, k + 1) for k, block in enumerate(sent)]
    return call(total_kernel, place, (keep, *got), [shape(ROWS, COLS)])[0], sent[0]


def adam_update(weights, first_moment, second_moment, gradient):
    first_new = beta_one * first_moment + (1.0 - beta_one) * gradient
    second_new = beta_two * second_moment + (1.0 - beta_two) * gradient * gradient
    corrected = first_new * (1.0 / (1.0 - beta_one**STEP))
    scaled = jnp.sqrt(second_new * (1.0 / (1.0 - beta_two**STEP))) + adam_eps
    weights_new = weights - learn_rate * (corrected / scaled + decay_rate * weights)
    return (weights_new, first_new, second_new)


def gradient_and_state(place, pair, half, states, rows, s):
    here, there = states
    columns = slice(s * PART, (s + 1) * PART)
    gradient = f32(pair[0][rows, columns]) + f32(pair[1][rows, columns])
    return gradient, [
        jnp.where(place[XH] == s, f32(here[half, k, rows]), f32(there[half, k, rows])) for k in range(3)
    ]


def adam_kernel(is_near, place, one, two, here, there, out):
    half = place[XL] if is_near else 1 - place[XL]

    def step(rows):
        for s in range(2):
            gradient, old = gradient_and_state(place, (one, two), half, (here, there), rows, s)
            out[rows, s * PART : (s + 1) * PART] = bf16(adam_update(*old, gradient)[0])

    in_rows(step)


def adam(place, is_near, pair, states):
    return call(functools.partial(adam_kernel, is_near), place, (*pair, *states), [shape(ROWS, COLS)])[0]


def adam_own_kernel(place, near, near_got, far, far_got, here, there, weights, first, second):
    def step(rows):
        is_near = place[XH] == place[XL]
        for s in range(2):
            columns = slice(s * PART, (s + 1) * PART)
            _, old = gradient_and_state(place, (near, near_got), place[XH], (here, there), rows, s)
            gradient = jnp.where(is_near, f32(near[rows, columns]), f32(far[rows, columns])) + jnp.where(
                is_near, f32(near_got[rows, columns]), f32(far_got[rows, columns])
            )
            for ref, value in zip((weights, first, second), adam_update(*old, gradient)):
                ref[rows, columns] = value

    in_rows(step)


def line_kernel(place, *refs):
    low, high = refs[4:]
    for behind in range(4):
        source = lax.rem(place[SECOND] + 4 - behind, 4)

        @pl.when(source < 2)
        def _():
            low[source] = refs[behind][...]

        @pl.when(source >= 2)
        def _():
            high[source - 2] = refs[behind][...]


def lay_kernel(is_near, steps, place, *refs):
    out, sems = refs[-2], refs[-1]
    x = place[XL] if is_near else 1 - place[XL]

    def copy(k, along_y):
        half, ahead = steps[k]
        other, pair = lax.rem(place[FIRST] + ahead, 4), pl.ds(2 * half, 2)
        index = (x, pair, other) if along_y else (x, other, pair)
        return pltpu.make_async_copy(refs[k], out.at[index], sems.at[k])

    for core in range(2):

        @pl.when(place[CORE] == core)
        def _():
            for k in range(len(steps)):
                copy(k, core == 0).start()
            for k in range(len(steps)):
                copy(k, core == 0).wait()


def lay(place, is_near, steps, pieces, *out):
    return call(
        functools.partial(lay_kernel, is_near, steps),
        place,
        [*pieces, *out],
        [shape(2, 4, 4, ROWS, COLS)],
        [pltpu.SemaphoreType.DMA((len(pieces),))],
        (pltpu.HBM,),
        len(out),
    )[0]


def lines(place, block):
    blocks = (block, *(ring(block, 1, k) for k in (1, 2, 3)))
    return call(line_kernel, place, blocks, [shape(2, ROWS, COLS)] * 2)


def gathered(place, line, is_near, *out):
    low, high = line
    low_up, high_down = ring(low, 0, 1), ring(high, 0, -1)
    high_up, low_down = ring(high, 0, 1), ring(low, 0, -1)
    far_up, far_down = ring(low_up, 0, 1), ring(high_down, 0, -1)
    steps = ((0, 0), (1, 0), (0, 3), (1, 1), (1, 3), (0, 1))
    out = lay(place, is_near, steps, (low, high, low_up, high_down, high_up, low_down), *out)
    return lay(place, is_near, ((0, 2), (1, 2)), (far_up, far_down), out)


def state_kernel(place, got, out, turned):
    def half(h, carry):
        for source in range(16):
            turned[source * 40 : (source + 1) * 40, :480] = f32(got[source, h])
        flat = turned[...].T
        for k in range(3):
            out[h, k] = bf16(flat[k * ROWS : (k + 1) * ROWS])
        return carry

    turned[:, 480:] = jnp.zeros((PART, 32), jnp.float32)
    lax.fori_loop(0, 2, half, 0)


def send_kernel(place, *refs):
    states, out = refs[:3], refs[3]

    def four(g, carry):
        for j in range(4):
            block = 4 * g + j
            for k, state in enumerate(states):
                rows = state[:, pl.ds(pl.multiple_of(g * 640, 128), 640)]
                out[lax.rem(block, 16), lax.div(block, 16), :, k * ROWS : (k + 1) * ROWS] = bf16(
                    rows[:, j * ROWS : (j + 1) * ROWS]
                )
        return carry

    lax.fori_loop(0, 8, four, 0)


def sent_state(place, states):
    return call(send_kernel, place, [s.T for s in states], [shape(16, 2, 40, 3 * ROWS)])[0]


def moved_state(place, flat):
    got = lax.all_to_all(flat, ("z", "y"), 0, 0, tiled=True)
    return call(
        state_kernel, place, (got,), [shape(2, 3, ROWS, PART)], [pltpu.VMEM((PART, 512), jnp.float32)]
    )[0]


def step(activations, cotangent, weights, first_moment, second_moment):
    place = [lax.axis_index(a) for a in ("xh", "z", "y", "xl", "c")]
    swapped = place[CORE] == 1
    place += [jnp.where(swapped, place[Z], place[Y]), jnp.where(swapped, place[Y], place[Z])]
    place = jnp.stack(place).astype(jnp.int32)
    across = shift(activations, "xl", 1)
    beside = shift(activations, "c", 1)
    flat = sent_state(place, (weights, first_moment, second_moment))
    here = moved_state(place, flat)
    messages = products(place, cotangent, activations, beside)
    near, sent = reduced(place, messages)

    across, here, _ = lax.optimization_barrier((across, here, sent))
    there = shift(here, "xh", 1)
    messages = products(place, cotangent, across, shift(across, "c", 1))
    near_got = shift(near, "xh", 1)
    near_line = lines(place, adam(place, True, (near, near_got), (here, there)))
    far, sent = reduced(place, messages)

    *near_line, _ = lax.optimization_barrier((*near_line, sent))
    out = gathered(place, near_line, True)
    far_got = shift(far, "xh", 1)
    block = adam(place, False, (far, far_got), (here, there))
    far_line = lines(place, block)
    out = gathered(place, far_line, False, out)
    weights_new, first_new, second_new = call(
        adam_own_kernel,
        place,
        (near, near_got, far, far_got, here, there),
        [shape(ROWS, COLS, dtype=jnp.float32)] * 3,
    )
    return (weights_new, first_new, second_new, out.reshape(D, COLS))


def solution(mesh):
    wide = Mesh(mesh.devices.reshape(2, 4, 4, 2, 2), ("xh", "z", "y", "xl", "c"))
    tensor = ("xl", "c")
    columns = P(None, (*tensor, *FSDP))
    rows = P(FSDP, tensor)
    return jax.shard_map(
        step,
        mesh=wide,
        in_specs=(rows, rows, columns, columns, columns),
        out_specs=(rows, rows, rows, P(None, tensor)),
        check_vma=False,
    )
```

```python
import functools

import jax
import jax.numpy as jnp
from jax import lax
from jax.experimental import pallas as pl
from jax.experimental.pallas import tpu as pltpu
from jax.sharding import Mesh, PartitionSpec as P

STEP = 20


beta_one = 0.9
beta_two = 0.95
adam_eps = 1e-08
learn_rate = 0.0003
decay_rate = 0.1

D = 5120
ROWS = 160
COLS = 1280
PART = 640
FSDP = ("xh", "z", "y")
VMEM_LIMIT = 12 * 1024 * 1024

XH, Z, Y, XL, CORE, FIRST, SECOND = range(7)


def f32(value):
    return value.astype(jnp.float32)


def bf16(value):
    return value.astype(jnp.bfloat16)


def shift(value, axis, step):
    count = lax.axis_size(axis)
    return lax.ppermute(value, axis, [(i, (i + step) % count) for i in range(count)])


def ring(value, second, step):
    pairs = []
    for z in range(4):
        for y in range(4):
            for core in range(2):
                along_y = core == second
                to = (z, (y + step) % 4) if along_y else ((z + step) % 4, y)
                pairs.append(((z * 4 + y) * 2 + core, (to[0] * 4 + to[1]) * 2 + core))
    return lax.ppermute(value, ("z", "y", "c"), pairs)


def shape(*dims, dtype=jnp.bfloat16):
    return jax.ShapeDtypeStruct(dims, dtype)


def call(kernel, place, args, outs, scratch=(), out_spaces=None, aliased=0):
    vmem = pl.BlockSpec(memory_space=pltpu.VMEM)
    there = [pl.BlockSpec(memory_space=space) for space in out_spaces or (pltpu.VMEM,) * len(outs)]
    held = len(args) - aliased
    return pl.pallas_call(
        kernel,
        out_shape=outs,
        in_specs=[pl.BlockSpec(memory_space=pltpu.SMEM)] + [vmem] * held + there[:aliased],
        out_specs=there,
        scratch_shapes=scratch,
        input_output_aliases={1 + held + i: i for i in range(aliased)},
        compiler_params=pltpu.CompilerParams(vmem_limit_bytes=VMEM_LIMIT),
    )(place, *args)


def in_rows(step):
    def run(i, carry):
        step(pl.ds(pl.multiple_of(i * 32, 32), 32))
        return carry

    lax.fori_loop(0, ROWS // 32, run, 0)


def multiply(features, cotangent, blocks):
    def one(low_z, carry):
        result = lax.dot_general(
            features[:, pl.ds(pl.multiple_of(low_z * 640, 128), 640)],
            cotangent[...],
            (((0,), (0,)), ((), ())),
            preferred_element_type=jnp.float32,
        )
        for j in range(4):
            blocks[low_z, j] = bf16(result[j * ROWS : (j + 1) * ROWS])
        return carry

    lax.fori_loop(0, 2, one, 0)


def first_product_kernel(place, features, cotangent, made):
    multiply(features, cotangent, made)


def product_kernel(place, made, features, cotangent, *refs):
    far_up, far_down, hold_up, hold_down, own, near_up, near_down, blocks, sems = refs
    multiply(features, cotangent, blocks)

    def send(value, ref, k):
        pltpu.make_async_copy(value, ref, sems.at[k]).start()

    def over_y(values, owner, low_z):
        def y_block(steps):
            return values.at[low_z, lax.rem(place[Y] + steps, 4)]

        send(y_block(0), own.at[2 * owner + low_z], 0)
        if owner == 0:
            send(y_block(3), near_down.at[low_z], 2)
            far_up[low_z] = y_block(2)[...]
            hold_up[low_z] = y_block(1)[...]
        else:
            send(y_block(1), near_up.at[low_z], 1)
            far_down[low_z] = y_block(2)[...]
            hold_down[low_z] = y_block(3)[...]

    def over_z(values, owner, low_z):
        ahead = lax.rem(2 * owner + low_z + 4 - place[Z], 4)

        @pl.when(ahead == 0)
        def _():
            send(values.at[low_z], own, 0)

        @pl.when(ahead == 1)
        def _():
            send(values.at[low_z, pl.ds(2, 2)], near_up, 1)
            hold_up[...] = values[low_z, :2]

        @pl.when(ahead == 2)
        def _():
            far_up[...] = values[low_z, :2]
            far_down[...] = values[low_z, 2:]

        @pl.when(ahead == 3)
        def _():
            send(values.at[low_z, pl.ds(0, 2)], near_down, 2)
            hold_down[...] = values[low_z, 2:]

    for core, arrange in ((0, over_y), (1, over_z)):

        @pl.when(place[CORE] == core)
        def _():
            for low_z in range(2):
                arrange(made, core, low_z)
                arrange(blocks, 1 - core, low_z)

    pltpu.make_async_copy(blocks.at[0], own, sems.at[0]).wait()
    pltpu.make_async_copy(blocks.at[0, pl.ds(0, 2)], near_up, sems.at[1]).wait()
    pltpu.make_async_copy(blocks.at[0, pl.ds(0, 2)], near_down, sems.at[2]).wait()


def products(place, cotangent, mine, other):
    made = call(first_product_kernel, place, (mine, cotangent), [shape(2, 4, ROWS, COLS)])[0]
    return call(
        product_kernel,
        place,
        (made, other, cotangent),
        [shape(n, ROWS, COLS) for n in (2, 2, 2, 2, 4, 2, 2)],
        [pltpu.VMEM((2, 4, ROWS, COLS), jnp.bfloat16), pltpu.SemaphoreType.DMA((3,))],
        (pltpu.VMEM,) * 4 + (pltpu.HBM,) * 3,
    )


def add_kernel(place, *refs):
    def step(rows):
        for k in range(2):
            for j in range(2):
                refs[4 + k][j, rows] = bf16(f32(refs[2 * k][j, rows]) + f32(refs[2 * k + 1][j, rows]))

    in_rows(step)


def pass_on(place, *blocks):
    return call(add_kernel, place, blocks, [shape(2, ROWS, COLS)] * 2)


def finish_kernel(place, own, near_down, last_up, near_up, last_down, *outs):
    def step(rows):
        for steps in range(4):
            to = lax.rem(place[SECOND] + steps, 4)
            first, second = jnp.minimum(to, 1), jnp.maximum(to - 2, 0)
            near = jnp.where(to < 2, f32(near_down[first, rows]), f32(near_up[second, rows]))
            last = jnp.where(to < 2, f32(last_up[first, rows]), f32(last_down[second, rows]))
            value = f32(own[to, rows]) + near + last
            outs[steps][rows] = value.astype(outs[steps].dtype)

    in_rows(step)


def finish(place, *blocks):
    kinds = (jnp.float32, jnp.bfloat16, jnp.bfloat16, jnp.bfloat16)
    return call(finish_kernel, place, blocks, [shape(ROWS, COLS, dtype=k) for k in kinds])


def total_kernel(place, keep, one, two, three, out):
    def step(rows):
        out[rows] = bf16(keep[rows] + f32(one[rows]) + f32(two[rows]) + f32(three[rows]))

    in_rows(step)


def reduced(place, messages):
    far_up, far_down, hold_up, hold_down, own, near_up, near_down = messages
    far_up, far_down = ring(far_up, 0, 1), ring(far_down, 0, -1)
    near_up, near_down = ring(near_up, 0, 1), ring(near_down, 0, -1)
    last_up, last_down = passed = pass_on(place, hold_up, far_up, hold_down, far_down)
    last_up, last_down = ring(last_up, 0, 1), ring(last_down, 0, -1)
    keep, *sent = finish(place, own, near_down, last_up, near_up, last_down)
    got = [ring(block, 1, k + 1) for k, block in enumerate(sent)]
    return call(total_kernel, place, (keep, *got), [shape(ROWS, COLS)])[0], passed[0], sent[0]


def adam_update(weights, first_moment, second_moment, gradient):
    first_new = beta_one * first_moment + (1.0 - beta_one) * gradient
    second_new = beta_two * second_moment + (1.0 - beta_two) * gradient * gradient
    corrected = first_new * (1.0 / (1.0 - beta_one**STEP))
    scaled = jnp.sqrt(second_new * (1.0 / (1.0 - beta_two**STEP))) + adam_eps
    weights_new = weights - learn_rate * (corrected / scaled + decay_rate * weights)
    return (weights_new, first_new, second_new)


def gradient_and_state(place, pair, half, states, rows, s):
    here, there = states
    columns = slice(s * PART, (s + 1) * PART)
    gradient = f32(pair[0][rows, columns]) + f32(pair[1][rows, columns])
    return gradient, [
        jnp.where(place[XH] == s, f32(here[half, k, rows]), f32(there[half, k, rows])) for k in range(3)
    ]


def adam_kernel(is_near, place, one, two, here, there, out):
    half = place[XL] if is_near else 1 - place[XL]

    def step(rows):
        for s in range(2):
            gradient, old = gradient_and_state(place, (one, two), half, (here, there), rows, s)
            out[rows, s * PART : (s + 1) * PART] = bf16(adam_update(*old, gradient)[0])

    in_rows(step)


def adam(place, is_near, pair, states):
    return call(functools.partial(adam_kernel, is_near), place, (*pair, *states), [shape(ROWS, COLS)])[0]


def adam_own_kernel(place, near, near_got, far, far_got, here, there, weights, first, second):
    def step(rows):
        is_near = place[XH] == place[XL]
        for s in range(2):
            columns = slice(s * PART, (s + 1) * PART)
            _, old = gradient_and_state(place, (near, near_got), place[XH], (here, there), rows, s)
            gradient = jnp.where(is_near, f32(near[rows, columns]), f32(far[rows, columns])) + jnp.where(
                is_near, f32(near_got[rows, columns]), f32(far_got[rows, columns])
            )
            for ref, value in zip((weights, first, second), adam_update(*old, gradient)):
                ref[rows, columns] = value

    in_rows(step)


def line_kernel(place, *refs):
    low, high = refs[4:]
    for behind in range(4):
        source = lax.rem(place[SECOND] + 4 - behind, 4)

        @pl.when(source < 2)
        def _():
            low[source] = refs[behind][...]

        @pl.when(source >= 2)
        def _():
            high[source - 2] = refs[behind][...]


def lay_kernel(is_near, steps, place, *refs):
    out, sems = refs[-2], refs[-1]
    x = place[XL] if is_near else 1 - place[XL]

    def copy(k, along_y):
        half, ahead = steps[k]
        other, pair = lax.rem(place[FIRST] + ahead, 4), pl.ds(2 * half, 2)
        index = (x, pair, other) if along_y else (x, other, pair)
        return pltpu.make_async_copy(refs[k], out.at[index], sems.at[k])

    for core in range(2):

        @pl.when(place[CORE] == core)
        def _():
            for k in range(len(steps)):
                copy(k, core == 0).start()
            for k in range(len(steps)):
                copy(k, core == 0).wait()


def lay(place, is_near, steps, pieces, *out):
    return call(
        functools.partial(lay_kernel, is_near, steps),
        place,
        [*pieces, *out],
        [shape(2, 4, 4, ROWS, COLS)],
        [pltpu.SemaphoreType.DMA((len(pieces),))],
        (pltpu.HBM,),
        len(out),
    )[0]


def lines(place, block):
    blocks = (block, *(ring(block, 1, k) for k in (1, 2, 3)))
    return call(line_kernel, place, blocks, [shape(2, ROWS, COLS)] * 2)


def gathered(place, line, is_near, *out):
    low, high = line
    low_up, high_down = ring(low, 0, 1), ring(high, 0, -1)
    high_up, low_down = ring(high, 0, 1), ring(low, 0, -1)
    far_up, far_down = ring(low_up, 0, 1), ring(high_down, 0, -1)
    steps = ((0, 0), (1, 0), (0, 3), (1, 1), (1, 3), (0, 1))
    out = lay(place, is_near, steps, (low, high, low_up, high_down, high_up, low_down), *out)
    return lay(place, is_near, ((0, 2), (1, 2)), (far_up, far_down), out)


def state_kernel(place, got, out, turned):
    def half(h, carry):
        for source in range(16):
            turned[source * 40 : (source + 1) * 40, :480] = f32(got[source, h])
        flat = turned[...].T
        for k in range(3):
            out[h, k] = bf16(flat[k * ROWS : (k + 1) * ROWS])
        return carry

    turned[:, 480:] = jnp.zeros((PART, 32), jnp.float32)
    lax.fori_loop(0, 2, half, 0)


def send_kernel(place, *refs):
    states, out = refs[:3], refs[3]

    def four(g, carry):
        for j in range(4):
            block = 4 * g + j
            for k, state in enumerate(states):
                rows = state[:, pl.ds(pl.multiple_of(g * 640, 128), 640)]
                out[lax.rem(block, 16), lax.div(block, 16), :, k * ROWS : (k + 1) * ROWS] = bf16(
                    rows[:, j * ROWS : (j + 1) * ROWS]
                )
        return carry

    lax.fori_loop(0, 8, four, 0)


def sent_state(place, states):
    return call(send_kernel, place, [s.T for s in states], [shape(16, 2, 40, 3 * ROWS)])[0]


def moved_state(place, flat):
    got = lax.all_to_all(flat, ("z", "y"), 0, 0, tiled=True)
    return call(
        state_kernel, place, (got,), [shape(2, 3, ROWS, PART)], [pltpu.VMEM((PART, 512), jnp.float32)]
    )[0]


def step(activations, cotangent, weights, first_moment, second_moment):
    place = [lax.axis_index(a) for a in ("xh", "z", "y", "xl", "c")]
    swapped = place[CORE] == 1
    place += [jnp.where(swapped, place[Z], place[Y]), jnp.where(swapped, place[Y], place[Z])]
    place = jnp.stack(place).astype(jnp.int32)
    across = shift(activations, "xl", 1)
    beside = shift(activations, "c", 1)
    flat = sent_state(place, (weights, first_moment, second_moment))
    here = moved_state(place, flat)
    messages = products(place, cotangent, activations, beside)
    near, passed, _ = reduced(place, messages)

    across, here, _ = lax.optimization_barrier((across, here, passed))
    there = shift(here, "xh", 1)
    messages = products(place, cotangent, across, shift(across, "c", 1))
    near_got = shift(near, "xh", 1)
    near_line = lines(place, adam(place, True, (near, near_got), (here, there)))
    far, _, sent = reduced(place, messages)

    *near_line, _ = lax.optimization_barrier((*near_line, sent))
    out = gathered(place, near_line, True)
    far_got = shift(far, "xh", 1)
    block = adam(place, False, (far, far_got), (here, there))
    far_line = lines(place, block)
    out = gathered(place, far_line, False, out)
    weights_new, first_new, second_new = call(
        adam_own_kernel,
        place,
        (near, near_got, far, far_got, here, there),
        [shape(ROWS, COLS, dtype=jnp.float32)] * 3,
    )
    return (weights_new, first_new, second_new, out.reshape(D, COLS))


def solution(mesh):
    wide = Mesh(mesh.devices.reshape(2, 4, 4, 2, 2), ("xh", "z", "y", "xl", "c"))
    tensor = ("xl", "c")
    columns = P(None, (*tensor, *FSDP))
    rows = P(FSDP, tensor)
    return jax.shard_map(
        step,
        mesh=wide,
        in_specs=(rows, rows, columns, columns, columns),
        out_specs=(rows, rows, rows, P(None, tensor)),
        check_vma=False,
    )
```
